32 devices in a mesh: group: 4 (over y, x), replica: 8 (over z, core).
Axes of the slice: x: 2, y: 2, z: 4, core: 2. Of those that a mesh axis runs over, the one named last changes fastest.
Arguments:
- inputs: bfloat16 [4096, 2048], P(('group', 'replica')), may hold values from -6 to 6
- cotangent: bfloat16 [4096, 2048], P(('group', 'replica')), may hold values from -6 to 6
- block_map: int32 [4, 8], P('group'), may hold values from 0 to 7, as said below
- positions: int32 [4096], P(('group', 'replica')), may hold values from 0 to 1023, as said below
- step_count: int32 [1], replicated, may hold values from 1 to 20
- weight_qkv: float32 [2048, 4096], P(('group', 'replica')), may hold values from -0.125 to 0.125
- first_qkv: float32 [2048, 4096], P(('group', 'replica')), may hold values from -6 to 6
- second_qkv: float32 [2048, 4096], P(('group', 'replica')), may hold values from 64 to 1024
- weight_out: float32 [2048, 2048], P(('group', 'replica')), may hold values from -1.5 to 1.5
- first_out: float32 [2048, 2048], P(('group', 'replica')), may hold values from -6 to 6
- second_out: float32 [2048, 2048], P(('group', 'replica')), may hold values from 0.5 to 5
- weight_gate_up: float32 [2048, 12288], P(('group', 'replica')), may hold values from -0.125 to 0.125
- first_gate_up: float32 [2048, 12288], P(('group', 'replica')), may hold values from -6 to 6
- second_gate_up: float32 [2048, 12288], P(('group', 'replica')), may hold values from 0.5 to 5
- weight_down: float32 [6144, 2048], P(('group', 'replica')), may hold values from -0.078125 to 0.078125
- first_down: float32 [6144, 2048], P(('group', 'replica')), may hold values from -6 to 6
- second_down: float32 [6144, 2048], P(('group', 'replica')), may hold values from 0.5 to 5
- norm_gains: float32 [4352], P(('group', 'replica')), may hold values from 0.5 to 1.5
- first_gains: float32 [4352], P(('group', 'replica')), may hold values from -6 to 6
- second_gains: float32 [4352], P(('group', 'replica')), may hold values from 64 to 1024
Outputs:
- block_out: bfloat16 [4096, 2048], P(('group', 'replica'))
- input_grad: float32 [4096, 2048], P(('group', 'replica'))
- grad_qkv: float32 [2048, 4096], P(('group', 'replica'))
- grad_out: float32 [2048, 2048], P(('group', 'replica'))
- grad_gate_up: float32 [2048, 12288], P(('group', 'replica'))
- grad_down: float32 [6144, 2048], P(('group', 'replica'))
- grad_gains: float32 [4352], P(('group', 'replica'))
- new_qkv: float32 [2048, 4096], P(('group', 'replica'))
- new_first_qkv: float32 [2048, 4096], P(('group', 'replica'))
- new_second_qkv: float32 [2048, 4096], P(('group', 'replica'))
- new_out: float32 [2048, 2048], P(('group', 'replica'))
- new_first_out: float32 [2048, 2048], P(('group', 'replica'))
- new_second_out: float32 [2048, 2048], P(('group', 'replica'))
- new_gate_up: float32 [2048, 12288], P(('group', 'replica'))
- new_first_gate_up: float32 [2048, 12288], P(('group', 'replica'))
- new_second_gate_up: float32 [2048, 12288], P(('group', 'replica'))
- new_down: float32 [6144, 2048], P(('group', 'replica'))
- new_first_down: float32 [6144, 2048], P(('group', 'replica'))
- new_second_down: float32 [6144, 2048], P(('group', 'replica'))
- new_gains: float32 [4352], P(('group', 'replica'))
- new_first_gains: float32 [4352], P(('group', 'replica'))
- new_second_gains: float32 [4352], P(('group', 'replica'))
The draws below stay inside these ranges and needn't reach their ends.
Inputs may be any that keep to these rules, and one draw needn't show every extreme that they name: Each row is a permutation: slot s of group g holds tokens block_map[g, s] * 128 to block_map[g, s] * 128 + 127 of the group's 1 sequence laid end to end. Within each sequence, in token order, positions count up from 0 and restart at 0 at most once; some sequence has no restart.
All inputs are finite; a program needn't handle non-finite values.
Results may differ from the reference program's by a relative error of at most 0.04.
The reference program's roundings to bfloat16 on the way count: a program that leaves them out, or rounds other values in their place, can miss the bound.
Values may be sent and summed in bfloat16 or wider, within the bound.
A program may use at most 576 MiB of HBM per device.

```python
import math
import jax
import jax.numpy as jnp
from jax import lax

D = 2048
H = 16
KVH = 8
HD = 128
FF = 6144
C = 128
SPG = 1
SLOTS = 8
GROUP_TOK = 1024
SEQ = 1024
TOKENS = 4096
QKV_W = 4096
N_GROUP = 4


def block_orders(key):
    group_keys = jax.random.split(jax.random.fold_in(key, 101), N_GROUP)
    return jax.vmap(lambda one_key: jax.random.permutation(one_key, SLOTS))(group_keys).astype(jnp.int32)


def draw_block_map(key, part):
    return block_orders(key)


def draw_positions(key, part):
    orders = block_orders(key)
    restarts = jax.random.randint(jax.random.fold_in(key, 202), (N_GROUP * SPG,), 1, SEQ).astype(jnp.int32)
    chosen = jax.random.randint(jax.random.fold_in(key, 303), (), 0, N_GROUP * SPG)
    restarts = jnp.where(jnp.arange(N_GROUP * SPG) == chosen, SEQ, restarts).astype(jnp.int32).reshape(N_GROUP, SPG)
    token_ids = jnp.arange(GROUP_TOK, dtype=jnp.int32)
    ordinals = orders[:, token_ids // C] * C + (token_ids % C)[None, :]
    sequence_ids = ordinals // SEQ
    inner_pos = ordinals % SEQ
    cut_point = jnp.take_along_axis(restarts, sequence_ids, axis=1)
    return jnp.where(inner_pos < cut_point, inner_pos, inner_pos - cut_point).reshape(TOKENS).astype(jnp.int32)


def level_of(rng, shape, cuts, least, high):
    level = 1.0
    for dim, parts in cuts:
        heights = jax.random.uniform(jax.random.fold_in(jax.random.fold_in(rng, 6), dim), (parts,), jnp.float32, least / len(cuts), high / len(cuts))
        level = level * jnp.repeat(jnp.exp(heights), shape[dim] // parts).reshape((-1,) + (1,) * (len(shape) - 1 - dim))
    return level


def gaussian(key, shape, scale, reach, cuts=(), kind=jnp.bfloat16):
    values = jax.random.normal(key, shape, jnp.float32) * scale
    if len(cuts) > 0:
        values = level_of(key, shape, cuts, -0.22, 0.18) * values
    return jnp.clip(values, min=-reach, max=reach).astype(kind)


def setup_inputs(seed: int = 0) -> dict:
    streams_of = jax.random.split(jax.random.key(seed), 21)
    inputs = gaussian(streams_of[0], (TOKENS, D), 1.0, 6.0, ((0, 32),))
    cotangent = gaussian(streams_of[1], (TOKENS, D), 1.0, 6.0, ((0, 32),))
    block_map = draw_block_map(jax.random.fold_in(streams_of[20], 71), 0)
    positions = draw_positions(jax.random.fold_in(streams_of[20], 71), 0)
    step_count = jax.random.randint(streams_of[4], (1,), 1, 21).astype(jnp.int32)
    weight_qkv = gaussian(streams_of[5], (D, QKV_W), D ** -0.5, 0.125, ((0, 32),), jnp.float32)
    first_qkv = gaussian(streams_of[6], (D, QKV_W), 1.0, 6.0, ((0, 32),), jnp.float32)
    second_qkv = jnp.clip(jnp.exp(math.log(1024.0) - 2.7725887 * jax.random.uniform(streams_of[7], (D, QKV_W), jnp.float32) ** level_of(streams_of[7], (D, QKV_W), ((0, 32),), -0.2, 0.2)), 64.0, 1024.0)
    weight_out = gaussian(streams_of[8], (H * HD, D), 16 ** -0.5, 1.5, ((0, 32),), jnp.float32)
    first_out = gaussian(streams_of[9], (H * HD, D), 1.0, 6.0, ((0, 32),), jnp.float32)
    second_out = jnp.clip(jnp.exp(math.log(5.0) - 2.3025851 * jax.random.uniform(streams_of[10], (H * HD, D), jnp.float32) ** level_of(streams_of[10], (H * HD, D), ((0, 32),), -0.2, 0.2)), 0.5, 5.0)
    weight_gate_up = gaussian(streams_of[11], (D, 2 * FF), D ** -0.5, 0.125, ((0, 32),), jnp.float32)
    first_gate_up = gaussian(streams_of[12], (D, 2 * FF), 1.0, 6.0, ((0, 32),), jnp.float32)
    second_gate_up = jnp.clip(jnp.exp(math.log(5.0) - 2.3025851 * jax.random.uniform(streams_of[13], (D, 2 * FF), jnp.float32) ** level_of(streams_of[13], (D, 2 * FF), ((0, 32),), -0.2, 0.2)), 0.5, 5.0)
    weight_down = gaussian(streams_of[14], (FF, D), FF ** -0.5, 0.078125, ((0, 32),), jnp.float32)
    first_down = gaussian(streams_of[15], (FF, D), 1.0, 6.0, ((0, 32),), jnp.float32)
    second_down = jnp.clip(jnp.exp(math.log(5.0) - 2.3025851 * jax.random.uniform(streams_of[16], (FF, D), jnp.float32) ** level_of(streams_of[16], (FF, D), ((0, 32),), -0.2, 0.2)), 0.5, 5.0)
    norm_gains = jnp.clip(1.0 + 0.1 * jax.random.normal(streams_of[17], (2 * D + 2 * HD,), jnp.float32), 0.5, 1.5)
    first_gains = gaussian(streams_of[18], (2 * D + 2 * HD,), 1.0, 6.0, ((0, 32),), jnp.float32)
    second_gains = jnp.clip(jnp.exp(math.log(1024.0) - 2.7725887 * jax.random.uniform(streams_of[19], (2 * D + 2 * HD,), jnp.float32) ** level_of(streams_of[19], (2 * D + 2 * HD,), ((0, 32),), -0.2, 0.2)), 64.0, 1024.0)
    return {"inputs": inputs, "cotangent": cotangent, "block_map": block_map, "positions": positions, "step_count": step_count, "weight_qkv": weight_qkv, "first_qkv": first_qkv, "second_qkv": second_qkv, "weight_out": weight_out, "first_out": first_out, "second_out": second_out, "weight_gate_up": weight_gate_up, "first_gate_up": first_gate_up, "second_gate_up": second_gate_up, "weight_down": weight_down, "first_down": first_down, "second_down": second_down, "norm_gains": norm_gains, "first_gains": first_gains, "second_gains": second_gains}


norm_eps = 1e-06
rope_base = 1000000.0
learn_rate = 0.1
beta_first = 0.9
beta_second = 0.95
adam_eps = 1e-08
decay_rate = 0.1

def rounded(values):
    return lax.optimization_barrier(values.astype(jnp.bfloat16)).astype(jnp.float32)

def rms_scale(values):
    return lax.rsqrt(lax.optimization_barrier(jnp.mean(values * values, axis=-1, keepdims=True)) + norm_eps)

def norm_back(grad_normed, normed, scale):
    return scale * (grad_normed - normed * lax.optimization_barrier(jnp.mean(grad_normed * normed, axis=-1, keepdims=True)))

def rope_tables(token_pos):
    half_dim = HD // 2
    frequency = rope_base ** (-(jnp.arange(half_dim).astype(jnp.float32) * 2.0 / HD))
    angles = token_pos.astype(jnp.float32)[:, None] * frequency[None, :]
    return (jnp.cos(angles)[:, None, :], jnp.sin(angles)[:, None, :])

def rotate(vectors, cosine, sine_table):
    half_dim = vectors.shape[-1] // 2
    first_half = vectors[..., :half_dim]
    second_half = vectors[..., half_dim:]
    return jnp.concatenate([first_half * cosine - second_half * sine_table, second_half * cosine + first_half * sine_table], axis=-1)

def unrotate(gradients, cosine, sine_table):
    half_dim = gradients.shape[-1] // 2
    first_half = gradients[..., :half_dim]
    second_half = gradients[..., half_dim:]
    return jnp.concatenate([first_half * cosine + second_half * sine_table, second_half * cosine - first_half * sine_table], axis=-1)

def visible(query_ord, key_ord, seq_len):
    same_sequence = key_ord[None, :] // seq_len == query_ord[:, None] // seq_len
    return same_sequence & (key_ord[None, :] <= query_ord[:, None])

def adam_step(weight, first_moment, second, gradient, step_value, decay_value):
    new_first = beta_first * first_moment + (1.0 - beta_first) * gradient
    new_second = beta_second * second + (1.0 - beta_second) * gradient * gradient
    first_hat = new_first / (1.0 - beta_first ** step_value)
    second_hat = new_second / (1.0 - beta_second ** step_value)
    new_weight = weight - learn_rate * (first_hat / (jnp.sqrt(second_hat) + adam_eps) + decay_value * weight)
    return (new_weight, new_first, new_second)

def reference(inputs, cotangent, block_map, positions, step_count, weight_qkv, first_qkv, second_qkv, weight_out, first_out, second_out, weight_gate_up, first_gate_up, second_gate_up, weight_down, first_down, second_down, norm_gains, first_gains, second_gains):
    head_ratio = H // KVH
    attn_scale = HD ** (-0.5)
    seq_len = SEQ
    qkv_full = weight_qkv.astype(jnp.bfloat16)
    out_full = weight_out.astype(jnp.bfloat16)
    gu_full = weight_gate_up.astype(jnp.bfloat16)
    down_full = weight_down.astype(jnp.bfloat16)
    gain_values = rounded(norm_gains)
    gain_one = gain_values[:D]
    gain_two = gain_values[D:2 * D]
    gain_query = gain_values[2 * D:2 * D + HD]
    gain_key = gain_values[2 * D + HD:]
    blocks = min(GROUP_TOK, 1024)
    block_count = GROUP_TOK // blocks

    def one_group(totals, group_data):
        group_inputs, group_cot, map_row, group_pos = group_data
        token_ids = jnp.arange(GROUP_TOK, dtype=jnp.int32)
        ordinals = (jnp.take(map_row, token_ids // C).astype(jnp.int32) * C + token_ids % C).astype(jnp.int32)
        inputs_f = group_inputs.astype(jnp.float32)
        scale_one = rms_scale(inputs_f)
        normed_one = inputs_f * scale_one
        hidden_one = (normed_one * gain_one).astype(jnp.bfloat16)
        projected = jnp.dot(hidden_one, qkv_full, preferred_element_type=jnp.float32)
        query_raw = projected[:, :H * HD].reshape(GROUP_TOK, H, HD)
        key_raw = projected[:, H * HD:(H + KVH) * HD].reshape(GROUP_TOK, KVH, HD)
        value_rows = projected[:, (H + KVH) * HD:].reshape(GROUP_TOK, KVH, HD).astype(jnp.bfloat16)
        cosine, sine_table = rope_tables(group_pos)
        query_scale = rms_scale(query_raw)
        query_hat = query_raw * query_scale
        key_scale = rms_scale(key_raw)
        key_hat = key_raw * key_scale
        query_rot = (rotate(query_hat * gain_query, cosine, sine_table) * attn_scale).astype(jnp.bfloat16)
        key_rot = rotate(key_hat * gain_key, cosine, sine_table).astype(jnp.bfloat16)
        query_f = query_rot.astype(jnp.float32).reshape(GROUP_TOK, KVH, head_ratio, HD)
        key_f = key_rot.astype(jnp.float32)
        value_f = value_rows.astype(jnp.float32)

        def attend(block_id):
            row_start = (block_id * blocks).astype(jnp.int32)
            query_block = lax.dynamic_slice_in_dim(query_f, row_start, blocks, 0)
            order_block = lax.dynamic_slice_in_dim(ordinals, row_start, blocks, 0)
            allowed = visible(order_block, ordinals, seq_len)
            scores = jnp.einsum('qgrd,kgd->grqk', query_block, key_f)
            scores = jnp.where(allowed, scores, -1e+30)
            row_max = lax.optimization_barrier(jnp.max(scores, axis=-1, keepdims=True))
            attn_probs = jnp.where(allowed, jnp.exp(scores - row_max), 0.0)
            row_sum = lax.optimization_barrier(jnp.sum(attn_probs, axis=-1, keepdims=True))
            mixed_block = jnp.einsum('grqk,kgd->grqd', rounded(attn_probs), value_f) / row_sum
            return (mixed_block, (row_max + jnp.log(row_sum))[..., 0])
        mixed_blocks, lse_blocks = lax.map(attend, jnp.arange(block_count, dtype=jnp.int32))
        mixed_rows = mixed_blocks.transpose(0, 3, 1, 2, 4).reshape(GROUP_TOK, H * HD).astype(jnp.bfloat16)
        resid_one = inputs_f + jnp.dot(mixed_rows, out_full, preferred_element_type=jnp.float32)
        scale_two = rms_scale(resid_one)
        normed_two = resid_one * scale_two
        hidden_two = (normed_two * gain_two).astype(jnp.bfloat16)
        gate_up = jnp.dot(hidden_two, gu_full, preferred_element_type=jnp.float32)
        gate_in = gate_up[:, :FF]
        up_in = gate_up[:, FF:]
        sigmoid_gate = jax.nn.sigmoid(gate_in)
        silu_gate = gate_in * sigmoid_gate
        activated = (silu_gate * up_in).astype(jnp.bfloat16)
        block_out = (resid_one + jnp.dot(activated, down_full, preferred_element_type=jnp.float32)).astype(jnp.bfloat16)
        act_grad = jnp.dot(group_cot, down_full.T, preferred_element_type=jnp.float32)
        grad_down_part = jnp.dot(activated.T, group_cot, preferred_element_type=jnp.float32)
        gate_grad = act_grad * up_in * sigmoid_gate * (1.0 + gate_in * (1.0 - sigmoid_gate))
        up_grad = act_grad * silu_gate
        gate_up_grad = jnp.concatenate([gate_grad, up_grad], axis=1).astype(jnp.bfloat16)
        grad_gate_up_part = jnp.dot(hidden_two.T, gate_up_grad, preferred_element_type=jnp.float32)
        hidden_two_grad = jnp.dot(gate_up_grad, gu_full.T, preferred_element_type=jnp.float32)
        gain_two_grad = lax.optimization_barrier(jnp.sum(hidden_two_grad * normed_two, axis=0))
        resid_grad = group_cot.astype(jnp.float32) + norm_back(hidden_two_grad * gain_two, normed_two, scale_two)
        attn_grad = resid_grad.astype(jnp.bfloat16)
        grad_out_part = jnp.dot(mixed_rows.T, attn_grad, preferred_element_type=jnp.float32)
        mixed_grad = jnp.dot(attn_grad, out_full.T, preferred_element_type=jnp.float32).astype(jnp.bfloat16)
        mixed_grad_f = mixed_grad.astype(jnp.float32).reshape(GROUP_TOK, KVH, head_ratio, HD)
        row_delta = lax.optimization_barrier(jnp.sum(mixed_grad_f * mixed_rows.astype(jnp.float32).reshape(GROUP_TOK, KVH, head_ratio, HD), axis=-1))

        def back_block(carried, block_id):
            key_grad, value_grad = carried
            row_start = (block_id * blocks).astype(jnp.int32)
            query_block = lax.dynamic_slice_in_dim(query_f, row_start, blocks, 0)
            grad_block = lax.dynamic_slice_in_dim(mixed_grad_f, row_start, blocks, 0)
            delta_block = lax.dynamic_slice_in_dim(row_delta, row_start, blocks, 0).transpose(1, 2, 0)
            order_block = lax.dynamic_slice_in_dim(ordinals, row_start, blocks, 0)
            allowed = visible(order_block, ordinals, seq_len)
            scores = jnp.einsum('qgrd,kgd->grqk', query_block, key_f)
            attn_probs = jnp.where(allowed, jnp.exp(scores - lse_blocks[block_id][..., None]), 0.0)
            value_grad = value_grad + jnp.einsum('grqk,qgrd->kgd', rounded(attn_probs), grad_block)
            prob_grad = jnp.einsum('qgrd,kgd->grqk', grad_block, value_f)
            score_grad = rounded(attn_probs * (prob_grad - delta_block[..., None]))
            query_grad = jnp.einsum('grqk,kgd->qgrd', score_grad, key_f)
            key_grad = key_grad + jnp.einsum('grqk,qgrd->kgd', score_grad, query_block)
            return ((key_grad, value_grad), query_grad)
        zero_keys = jnp.zeros((GROUP_TOK, KVH, HD), jnp.float32)
        (key_grad, value_grad), query_grad_blocks = lax.scan(back_block, (zero_keys, zero_keys), jnp.arange(block_count, dtype=jnp.int32))
        query_grad = query_grad_blocks.reshape(GROUP_TOK, H, HD)
        query_norm_grad = unrotate(query_grad * attn_scale, cosine, sine_table)
        gain_query_grad = lax.optimization_barrier(jnp.sum(query_norm_grad * query_hat, axis=(0, 1)))
        query_raw_grad = norm_back(query_norm_grad * gain_query, query_hat, query_scale)
        key_norm_grad = unrotate(key_grad, cosine, sine_table)
        gain_key_grad = lax.optimization_barrier(jnp.sum(key_norm_grad * key_hat, axis=(0, 1)))
        key_raw_grad = norm_back(key_norm_grad * gain_key, key_hat, key_scale)
        projected_grad = jnp.concatenate([query_raw_grad.reshape(GROUP_TOK, H * HD), key_raw_grad.reshape(GROUP_TOK, KVH * HD), value_grad.reshape(GROUP_TOK, KVH * HD)], axis=1).astype(jnp.bfloat16)
        grad_qkv_part = jnp.dot(hidden_one.T, projected_grad, preferred_element_type=jnp.float32)
        hidden_one_grad = jnp.dot(projected_grad, qkv_full.T, preferred_element_type=jnp.float32)
        gain_one_grad = lax.optimization_barrier(jnp.sum(hidden_one_grad * normed_one, axis=0))
        input_grad = resid_grad + norm_back(hidden_one_grad * gain_one, normed_one, scale_one)
        grad_gains_part = jnp.concatenate([gain_one_grad, gain_two_grad, gain_query_grad, gain_key_grad])
        new_totals = (totals[0] + grad_qkv_part, totals[1] + grad_out_part, totals[2] + grad_gate_up_part, totals[3] + grad_down_part, totals[4] + grad_gains_part)
        return (new_totals, (block_out, input_grad))
    start_totals = (jnp.zeros((D, QKV_W), jnp.float32), jnp.zeros((H * HD, D), jnp.float32), jnp.zeros((D, 2 * FF), jnp.float32), jnp.zeros((FF, D), jnp.float32), jnp.zeros((2 * D + 2 * HD,), jnp.float32))
    group_data = (inputs.reshape(N_GROUP, GROUP_TOK, D), cotangent.reshape(N_GROUP, GROUP_TOK, D), block_map, positions.reshape(N_GROUP, GROUP_TOK))
    totals, (outs_all, grads_all) = lax.scan(one_group, start_totals, group_data)
    grad_qkv, grad_out, grad_gate_up, grad_down, grad_gains = totals
    step_value = step_count[0].astype(jnp.float32)
    new_qkv, new_first_qkv, new_second_qkv = adam_step(weight_qkv, first_qkv, second_qkv, grad_qkv, step_value, decay_rate)
    new_out, new_first_out, new_second_out = adam_step(weight_out, first_out, second_out, grad_out, step_value, decay_rate)
    new_gate_up, new_first_gate_up, new_second_gate_up = adam_step(weight_gate_up, first_gate_up, second_gate_up, grad_gate_up, step_value, decay_rate)
    new_down, new_first_down, new_second_down = adam_step(weight_down, first_down, second_down, grad_down, step_value, decay_rate)
    new_gains, new_first_gains, new_second_gains = adam_step(norm_gains, first_gains, second_gains, grad_gains, step_value, 0.0)
    return (outs_all.reshape(TOKENS, D), grads_all.reshape(TOKENS, D), grad_qkv, grad_out, grad_gate_up, grad_down, grad_gains, new_qkv, new_first_qkv, new_second_qkv, new_out, new_first_out, new_second_out, new_gate_up, new_first_gate_up, new_second_gate_up, new_down, new_first_down, new_second_down, new_gains, new_first_gains, new_second_gains)
```

```python
import jax
import jax.numpy as jnp
from jax import lax
from jax.sharding import PartitionSpec as P

HD = 128
KV_RATIO = 2
C = 128
SPG = 1

norm_eps = 1e-06
rope_base = 1000000.0
learn_rate = 0.1
beta_first = 0.9
beta_second = 0.95
adam_eps = 1e-08
decay_rate = 0.1
masked_score = -1e30
BF = jnp.bfloat16
F32 = jnp.float32


def rms_scale(values):
    return lax.rsqrt(jnp.mean(values * values, axis=-1, keepdims=True) + norm_eps)


def norm_back(grad_normed, normed, scale):
    return scale * (grad_normed - normed * jnp.mean(grad_normed * normed, axis=-1, keepdims=True))


def rope_tables(token_pos):
    half_dim = HD // 2
    frequency = rope_base ** (-(jnp.arange(half_dim).astype(F32) * 2.0 / HD))
    angles = token_pos.astype(F32)[:, None] * frequency[None, :]
    return (jnp.cos(angles)[:, None, :], jnp.sin(angles)[:, None, :])


def rotate(vectors, cosine, sine_table):
    half_dim = vectors.shape[-1] // 2
    first_half = vectors[..., :half_dim]
    second_half = vectors[..., half_dim:]
    return jnp.concatenate(
        [
            first_half * cosine - second_half * sine_table,
            second_half * cosine + first_half * sine_table,
        ],
        axis=-1,
    )


def unrotate(gradients, cosine, sine_table):
    return rotate(gradients, cosine, -sine_table)


def adam_step(weight, first_moment, second, gradient, step_value, decay_value):
    new_first = beta_first * first_moment + (1.0 - beta_first) * gradient
    new_second = beta_second * second + (1.0 - beta_second) * gradient * gradient
    first_hat = new_first / (1.0 - beta_first**step_value)
    second_hat = new_second / (1.0 - beta_second**step_value)
    new_weight = weight - learn_rate * (
        first_hat / (jnp.sqrt(second_hat) + adam_eps) + decay_value * weight
    )
    return (new_weight, new_first, new_second)


def dot(a, b):
    return jnp.dot(a, b, preferred_element_type=F32)


def dot_nt(a, b):
    return lax.dot_general(a, b, (((1,), (1,)), ((), ())), preferred_element_type=F32)


def dot_tn(a, b):
    return lax.dot_general(a, b, (((0,), (0,)), ((), ())), preferred_element_type=F32)


def gather_rows(block):
    return lax.all_gather(block, "replica", axis=0, tiled=True)


def scatter_rows(partial):
    return lax.psum_scatter(
        partial.astype(BF), "replica", scatter_dimension=0, tiled=True
    ).astype(F32)


def swap_blocks(blocks):
    return lax.all_to_all(blocks, "replica", 0, 0, tiled=True)


def make_local(groups, replicas):
    sub_count = replicas // groups
    sub_groups = [[s * groups + k for k in range(groups)] for s in range(sub_count)]
    slice_of = [(r % groups) * sub_count + r // groups for r in range(replicas)]

    def swap_sub(blocks):
        return lax.all_to_all(
            blocks, "replica", 0, 0, axis_index_groups=sub_groups, tiled=True
        )

    def gather_group(block):
        return lax.all_gather(block, "group", axis=0, tiled=True)

    def scatter_group(partial):
        return lax.psum_scatter(partial.astype(BF), "group", scatter_dimension=0, tiled=True)

    def local(
        inputs,
        cotangent,
        block_map,
        positions,
        step_count,
        weight_qkv,
        first_qkv,
        second_qkv,
        weight_out,
        first_out,
        second_out,
        weight_gate_up,
        first_gate_up,
        second_gate_up,
        weight_down,
        first_down,
        second_down,
        norm_gains,
        first_gains,
        second_gains,
    ):
        tok_rows, width = inputs.shape
        seq_rows = tok_rows * replicas
        own_rows = weight_qkv.shape[0]
        own_ff = weight_down.shape[0]
        heads = weight_out.shape[0] * groups * replicas // HD
        kv_heads = heads // KV_RATIO
        q_cols = heads * HD
        kv_cols = kv_heads * HD
        q_per = heads // replicas
        kv_per = max(1, kv_heads // replicas)
        ratio = q_per // kv_per
        kv_start = [slice_of[r] * q_per // KV_RATIO for r in range(replicas)]
        attn_scale = HD ** (-0.5)
        map_row = block_map[0]
        seq_len = map_row.shape[0] * C // SPG

        down_slice = gather_group(weight_down.astype(BF))
        qkv_b = weight_qkv.astype(BF)
        qkv_blocks = jnp.stack(
            [
                jnp.concatenate(
                    [
                        qkv_b[:, slice_of[r] * q_per * HD : (slice_of[r] + 1) * q_per * HD],
                        qkv_b[:, q_cols + kv_start[r] * HD : q_cols + (kv_start[r] + kv_per) * HD],
                        qkv_b[
                            :,
                            q_cols + kv_cols + kv_start[r] * HD : q_cols
                            + kv_cols
                            + (kv_start[r] + kv_per) * HD,
                        ],
                    ],
                    axis=1,
                )
                for r in range(replicas)
            ]
        )
        qkv_slice = gather_group(
            swap_blocks(qkv_blocks).reshape(replicas * own_rows, qkv_blocks.shape[2])
        )
        gu_blocks = (
            weight_gate_up.astype(BF)
            .reshape(own_rows, 2, groups, replicas, own_ff)
            .transpose(3, 0, 1, 2, 4)
            .reshape(replicas, own_rows, 2 * groups * own_ff)
        )
        gu_slice = gather_group(
            swap_blocks(gu_blocks).reshape(replicas * own_rows, gu_blocks.shape[2])
        )
        out_own = weight_out.shape[0]
        out_all = gather_group(weight_out.astype(BF)[None])
        out_slice = swap_sub(out_all).reshape(groups * out_own, width)
        ff_slice = groups * own_ff

        gains_full = lax.all_gather(
            norm_gains.astype(BF), ("group", "replica"), axis=0, tiled=True
        ).astype(F32)
        gain_one = gains_full[:width]
        gain_two = gains_full[width : 2 * width]
        gain_query = gains_full[2 * width : 2 * width + HD]
        gain_key = gains_full[2 * width + HD :]

        pos_all = lax.all_gather(positions, "replica", axis=0, tiled=True)
        row_ids = jnp.arange(seq_rows, dtype=jnp.int32)
        slot_hot = (row_ids // C)[:, None] == jnp.arange(map_row.shape[0], dtype=jnp.int32)[None, :]
        ordinals = (
            jnp.sum(jnp.where(slot_hot, map_row[None, :], 0), axis=1) * C + row_ids % C
        )
        allowed = (ordinals[None, :] // seq_len == ordinals[:, None] // seq_len) & (
            ordinals[None, :] <= ordinals[:, None]
        )
        cosine, sine_table = rope_tables(pos_all)

        x_all = gather_rows(inputs).astype(F32)
        cot_all = gather_rows(cotangent)
        hidden_one = (x_all * rms_scale(x_all) * gain_one).astype(BF)
        projected = dot(hidden_one, qkv_slice)
        query_raw = projected[:, : q_per * HD].reshape(seq_rows, q_per, HD)
        key_raw = projected[:, q_per * HD : (q_per + kv_per) * HD].reshape(seq_rows, kv_per, HD)
        value_rows = (
            projected[:, (q_per + kv_per) * HD :].reshape(seq_rows, kv_per, HD).astype(BF)
        )
        query_scale = rms_scale(query_raw)
        query_hat = query_raw * query_scale
        key_scale = rms_scale(key_raw)
        key_hat = key_raw * key_scale
        query_rot = (rotate(query_hat * gain_query, cosine, sine_table) * attn_scale).astype(BF)
        key_rot = rotate(key_hat * gain_key, cosine, sine_table).astype(BF)
        query_groups = query_rot.reshape(seq_rows, kv_per, ratio, HD)
        scores = jnp.einsum(
            "qgrd,kgd->grqk", query_groups, key_rot, preferred_element_type=F32
        )
        scores = jnp.where(allowed, scores, masked_score)
        row_max = jnp.max(scores, axis=-1)
        attn_probs = jnp.where(allowed, jnp.exp(scores - row_max[..., None]), 0.0)
        row_sum = jnp.sum(attn_probs, axis=-1)
        mixed_part = jnp.einsum(
            "grqk,kgd->grqd", attn_probs.astype(BF), value_rows, preferred_element_type=F32
        )
        log_total = row_max + jnp.log(row_sum)
        mixed = (
            (mixed_part / row_sum[..., None])
            .transpose(2, 0, 1, 3)
            .reshape(seq_rows, q_per * HD)
            .astype(BF)
        )
        x_own = inputs.astype(F32)
        resid_one = x_own + scatter_rows(dot(mixed, out_slice))
        scale_two = rms_scale(resid_one)
        normed_two = resid_one * scale_two
        hidden_two = gather_rows((normed_two * gain_two).astype(BF))

        gate_up = dot(hidden_two, gu_slice)
        gate_in = gate_up[:, :ff_slice]
        up_in = gate_up[:, ff_slice:]
        sigmoid_gate = jax.nn.sigmoid(gate_in)
        silu_gate = gate_in * sigmoid_gate
        activated = (silu_gate * up_in).astype(BF)
        block_part = dot(activated, down_slice)
        act_grad = dot_nt(cot_all, down_slice)
        gate_grad = act_grad * up_in * sigmoid_gate * (1.0 + gate_in * (1.0 - sigmoid_gate))
        up_grad = act_grad * silu_gate
        gate_up_grad = jnp.concatenate([gate_grad, up_grad], axis=1).astype(BF)
        hidden_two_grad = scatter_rows(dot_nt(gate_up_grad, gu_slice))
        block_out = (resid_one + scatter_rows(block_part)).astype(BF)
        gain_two_grad = jnp.sum(hidden_two_grad * normed_two, axis=0)
        resid_grad = cotangent.astype(F32) + norm_back(
            hidden_two_grad * gain_two, normed_two, scale_two
        )
        attn_grad = gather_rows(resid_grad.astype(BF))

        grad_down = scatter_group(dot_tn(activated, cot_all)).astype(F32)
        gu_mid = scatter_group(dot_tn(hidden_two, gate_up_grad))
        grad_gate_up = (
            swap_blocks(gu_mid.reshape(replicas, own_rows, 2 * ff_slice))
            .reshape(replicas, own_rows, 2, groups, own_ff)
            .transpose(1, 2, 3, 0, 4)
            .reshape(own_rows, 2 * groups * replicas * own_ff)
            .astype(F32)
        )

        mixed_grad = dot_nt(attn_grad, out_slice).astype(BF)
        grad_out_part = dot_tn(mixed, attn_grad).astype(BF).reshape(groups, out_own, width)
        grad_out = scatter_group(swap_sub(grad_out_part))[0].astype(F32)
        mixed_grad_groups = mixed_grad.reshape(seq_rows, kv_per, ratio, HD).transpose(1, 2, 0, 3)
        row_delta = jnp.sum(
            (mixed_grad.astype(F32) * mixed.astype(F32)).reshape(seq_rows, kv_per, ratio, HD),
            axis=-1,
        ).transpose(1, 2, 0)
        probs = jnp.where(allowed, jnp.exp(scores - log_total[..., None]), 0.0)
        value_grad = jnp.einsum(
            "grqk,grqd->kgd", probs.astype(BF), mixed_grad_groups, preferred_element_type=F32
        )
        prob_grad = jnp.einsum(
            "grqd,kgd->grqk", mixed_grad_groups, value_rows, preferred_element_type=F32
        )
        score_grad = (probs * (prob_grad - row_delta[..., None])).astype(BF)
        query_grad = jnp.einsum(
            "grqk,kgd->qgrd", score_grad, key_rot, preferred_element_type=F32
        ).reshape(seq_rows, q_per, HD)
        key_grad = jnp.einsum(
            "grqk,qgrd->kgd", score_grad, query_groups, preferred_element_type=F32
        )
        query_norm_grad = unrotate(query_grad * attn_scale, cosine, sine_table)
        gain_query_grad = jnp.sum(query_norm_grad * query_hat, axis=(0, 1))
        query_raw_grad = norm_back(query_norm_grad * gain_query, query_hat, query_scale)
        key_norm_grad = unrotate(key_grad, cosine, sine_table)
        gain_key_grad = jnp.sum(key_norm_grad * key_hat, axis=(0, 1))
        key_raw_grad = norm_back(key_norm_grad * gain_key, key_hat, key_scale)
        projected_grad = jnp.concatenate(
            [
                query_raw_grad.reshape(seq_rows, q_per * HD),
                key_raw_grad.reshape(seq_rows, kv_per * HD),
                value_grad.reshape(seq_rows, kv_per * HD),
            ],
            axis=1,
        ).astype(BF)
        qkv_mid = scatter_group(dot_tn(hidden_one, projected_grad))
        qkv_back = swap_blocks(qkv_mid.reshape(replicas, own_rows, qkv_mid.shape[1])).astype(F32)
        q_at = [slice_of.index(j) for j in range(replicas)]
        shares = [
            [r for r in range(replicas) if kv_start[r] <= m < kv_start[r] + kv_per]
            for m in range(kv_heads)
        ]

        def kv_part(offset):
            pieces = []
            for m in range(kv_heads):
                terms = [
                    qkv_back[r][
                        :,
                        offset + (m - kv_start[r]) * HD : offset + (m - kv_start[r] + 1) * HD,
                    ]
                    for r in shares[m]
                ]
                pieces.append(sum(terms[1:], terms[0]))
            return pieces

        grad_qkv = jnp.concatenate(
            [qkv_back[r][:, : q_per * HD] for r in q_at]
            + kv_part(q_per * HD)
            + kv_part((q_per + kv_per) * HD),
            axis=1,
        )
        hidden_one_grad = scatter_rows(dot_nt(projected_grad, qkv_slice))
        scale_one = rms_scale(x_own)
        normed_one = x_own * scale_one
        gain_one_grad = jnp.sum(hidden_one_grad * normed_one, axis=0)
        input_grad = resid_grad + norm_back(hidden_one_grad * gain_one, normed_one, scale_one)
        grad_gains_part = jnp.concatenate(
            [gain_one_grad, gain_two_grad, gain_query_grad, gain_key_grad]
        )
        grad_gains = lax.psum_scatter(
            grad_gains_part, ("group", "replica"), scatter_dimension=0, tiled=True
        )

        step_value = step_count[0].astype(F32)
        new_qkv = adam_step(weight_qkv, first_qkv, second_qkv, grad_qkv, step_value, decay_rate)
        new_out = adam_step(weight_out, first_out, second_out, grad_out, step_value, decay_rate)
        new_gu = adam_step(
            weight_gate_up, first_gate_up, second_gate_up, grad_gate_up, step_value, decay_rate
        )
        new_down = adam_step(
            weight_down, first_down, second_down, grad_down, step_value, decay_rate
        )
        new_gains = adam_step(norm_gains, first_gains, second_gains, grad_gains, step_value, 0.0)
        return (
            block_out,
            input_grad,
            grad_qkv,
            grad_out,
            grad_gate_up,
            grad_down,
            grad_gains,
            *new_qkv,
            *new_out,
            *new_gu,
            *new_down,
            *new_gains,
        )

    return local


def solution(mesh):
    both = ("group", "replica")
    rows = P(both, None)
    flat = P(both)
    in_specs = (rows, rows, P("group", None), flat, P()) + (rows,) * 12 + (flat,) * 3
    out_specs = (rows,) * 6 + (flat,) + (rows,) * 12 + (flat,) * 3
    local = make_local(mesh.shape["group"], mesh.shape["replica"])
    return jax.shard_map(local, mesh=mesh, in_specs=in_specs, out_specs=out_specs, check_vma=False)
```
